32 devices in a mesh: grp: 2 (over x), blk: 16 (over z, y, core).
Axes of the slice: x: 2, y: 2, z: 4, core: 2. Of those that a mesh axis runs over, the one named last changes fastest.
Arguments:
- sensors: float32 [3, 32768], P(None, 'blk'), may hold values from 0 to 1
- sources: bfloat16 [3, 65536], P(None, ('grp', 'blk')), may hold values from 0 to 1
- weights: bfloat16 [65536], P(('grp', 'blk')), may hold values from 0.5 to 2
- probes: bfloat16 [65536, 128], P(('grp', 'blk')), may hold values from -6 to 6
Outputs:
- response: float32 [128, 32768], P('grp', 'blk')
The draws below stay inside these ranges and needn't reach their ends.
All inputs are finite; a program needn't handle non-finite values.
Results may differ from the reference program's by a relative error of at most 0.01.
Values may be sent and summed in bfloat16 or wider, within the bound.
A program may use at most 64 MiB of HBM per device.

```python
import math
import jax
import jax.numpy as jnp
from jax import lax

SENS_DEV = 2048
SRC_DEV = 2048
PROBES = 128
STEPS = 6
SENSORS = 32768
SOURCES = 65536
N_GRP = 2
N_BLK = 16


def block_levels(stream_key, shape, pieces, smallest, largest):
    loudness, own = 1.0, jax.random.fold_in(stream_key, 6)
    for position, shards_of in pieces:
        steps = jnp.exp(jax.random.uniform(jax.random.fold_in(own, position), (shards_of,), jnp.float32, smallest / len(pieces), largest / len(pieces)))
        loudness = loudness * jnp.repeat(steps, shape[position] // shards_of).reshape([-1 if axis == position else 1 for axis in range(len(shape))])
    return loudness


def scatter_about(rng, extent, width, limit, shards=(), kind=jnp.bfloat16):
    values = jax.random.normal(rng, extent, jnp.float32) * width
    if len(shards) > 0:
        values = block_levels(rng, extent, shards, -0.22, 0.18) * values
    return jnp.clip(values, min=-limit, max=limit).astype(kind)


def setup_inputs(seed: int = 0) -> dict:
    key_of = jax.random.split(jax.random.key(seed), 5)
    return {
        "sensors": jnp.clip(1.0 * jax.random.uniform(key_of[0], (3, SENSORS), jnp.float32) ** block_levels(key_of[0], (3, SENSORS), ((1, 16),), -0.2, 0.2), 0.0, 1.0),
        "sources": jnp.clip(1.0 * jax.random.uniform(key_of[1], (3, SOURCES), jnp.float32) ** block_levels(key_of[1], (3, SOURCES), ((1, 32),), -0.2, 0.2), 0.0, 1.0).astype(jnp.bfloat16),
        "weights": jnp.clip(jnp.exp(math.log(2.0) - 1.3862944 * jax.random.uniform(key_of[2], (SOURCES,), jnp.float32) ** block_levels(key_of[2], (SOURCES,), ((0, 32),), -0.2, 0.2)), 0.5, 2.0).astype(jnp.bfloat16),
        "probes": scatter_about(key_of[3], (SOURCES, PROBES), 1.0, 6.0, ((0, 32),)),
    }


def kernel_tile(sens, src, wgt, prb):
    dist = jnp.zeros((src.shape[1], sens.shape[1]), jnp.float32)
    for comp in range(3):
        delta = src[comp].astype(jnp.float32)[:, None] - sens[comp][None, :]
        dist = dist + delta * delta
    ker = (wgt.astype(jnp.float32)[:, None] * lax.rsqrt(dist + 0.0025)).astype(jnp.bfloat16)
    return lax.dot_general(prb, ker, (((0,), (0,)), ((), ())), preferred_element_type=jnp.float32)

def reference(sensors, sources, weights, probes):
    srcs = sources.reshape(3, N_GRP, N_BLK, SRC_DEV)
    wgts = weights.reshape(N_GRP, N_BLK, SRC_DEV)
    prbs = probes.reshape(N_GRP, N_BLK, SRC_DEV, PROBES)
    sens_all = sensors.reshape(3, N_BLK, SENS_DEV)
    scale = 1.0 / math.sqrt(STEPS * SRC_DEV * N_GRP)

    def one_block(index):
        sens = lax.dynamic_index_in_dim(sens_all, index, 1, keepdims=False)
        total = jnp.zeros((PROBES, SENS_DEV), jnp.float32)
        for group in range(N_GRP):
            part = jnp.zeros((PROBES, SENS_DEV), jnp.float32)
            for step in range(STEPS):
                other = ((index - step) % N_BLK).astype(jnp.int32)
                src = lax.dynamic_index_in_dim(srcs[:, group], other, 1, keepdims=False)
                wgt = lax.dynamic_index_in_dim(wgts[group], other, 0, keepdims=False)
                prb = lax.dynamic_index_in_dim(prbs[group], other, 0, keepdims=False)
                part = part + kernel_tile(sens, src, wgt, prb)
            rounded = lax.optimization_barrier((part * scale).astype(jnp.bfloat16))
            total = total + rounded.astype(jnp.float32)
        return total
    blocks = lax.map(one_block, jnp.arange(N_BLK, dtype=jnp.int32))
    return jnp.transpose(blocks, (1, 0, 2)).reshape(PROBES, N_BLK * SENS_DEV)
```

```python
import functools
import math

import jax
import jax.numpy as jnp
from jax import lax
from jax.experimental import pallas as pl
from jax.experimental.pallas import tpu as pltpu
from jax.sharding import PartitionSpec as P

STEPS = 6
SLOTS = STEPS + 1
EPS = 0.0025
FEAT = 16
CHUNKS = 4
QUARTERS = 4
TILE = 256
MESH = pl.DeviceIdType.MESH


def pieces(x):
    hi = x.astype(jnp.bfloat16)
    rest = x - hi.astype(jnp.float32)
    mid = rest.astype(jnp.bfloat16)
    lo = (rest - mid.astype(jnp.float32)).astype(jnp.bfloat16)
    return [hi.astype(jnp.float32), mid.astype(jnp.float32), lo.astype(jnp.float32)]


def body(groups, n_blk, scale, sens_ref, src_ref, wgt_ref, prb_ref, out_ref,
         bufs, feat, acc, part, got, send_sem, recv_sem, psend_sem, precv_sem):
    chunk = bufs.shape[3]
    probes = prb_ref.shape[1]
    sensors = sens_ref.shape[1]
    rows = probes // groups
    quarter = sensors // QUARTERS
    chips = n_blk // 2

    grp = lax.axis_index("grp")
    me = lax.axis_index("blk")
    chip = me // 2
    core = me % 2
    odd = chip % 2
    ahead = 2 * ((chip + 2) % chips) + core
    behind = 2 * ((chip + chips - 2) % chips) + core
    peer = 2 * (chip + 1 - 2 * odd) + core
    twin = 2 * chip + 1 - core

    barrier = pltpu.get_barrier_semaphore()
    for other in (ahead, behind, peer, twin):
        pl.semaphore_signal(barrier, inc=1, device_id=(grp, other), device_id_type=MESH)
    for k in range(1, groups):
        pl.semaphore_signal(barrier, inc=1, device_id=((grp + k) % groups, me), device_id_type=MESH)

    for j in range(CHUNKS):
        cols = pl.ds(j * chunk, chunk)
        turned = jnp.transpose(prb_ref[cols, :].astype(jnp.float32))
        bufs[0, j, :probes, :] = (turned * wgt_ref[:, cols].astype(jnp.float32)).astype(jnp.bfloat16)
        s = src_ref[:, cols].astype(jnp.float32)
        square = jnp.sum(s * s, axis=0, keepdims=True)
        one = jnp.ones((1, chunk), jnp.float32)
        bufs[0, j, probes:, :] = jnp.concatenate(
            [s, s, s] + pieces(square) + [one, one, one, 0.0 * one], axis=0
        ).astype(jnp.bfloat16)
    x = sens_ref[...]
    square = jnp.sum(x * x, axis=0, keepdims=True) + EPS
    one = jnp.ones((1, sensors), jnp.float32)
    feat[...] = jnp.concatenate(
        [-2.0 * p for p in pieces(x)] + [one, one, one] + pieces(square) + [0.0 * one], axis=0
    ).astype(jnp.bfloat16)

    def copy(kind, src_slot, dst_slot, j, other):
        return pltpu.make_async_remote_copy(
            src_ref=bufs.at[src_slot, j],
            dst_ref=bufs.at[dst_slot, j],
            send_sem=send_sem.at[kind, j],
            recv_sem=recv_sem.at[dst_slot, j],
            device_id=(grp, other),
            device_id_type=MESH,
        )

    def arrived(slot, j):
        copy(0, slot, slot, j, ahead).wait_recv()

    def far(j): return copy(0, 0, 4, j, ahead)
    def near(j): return copy(1, 4 * odd, 2, j, peer)
    def relay_far(j): return copy(2, 2, 6, j, ahead)
    def relay_near(j): return copy(3, 4, 6, j, peer)
    def twin_own(j): return copy(4, 0, 1, j, twin)
    def twin_four(j): return copy(5, 4, 5 - 2 * core, j, twin)
    def twin_two(j): return copy(6, 2, 3 - 2 * core, j, twin)
    def twin_six(j): return copy(7, 6, 5, j, twin)

    relays = jnp.logical_and(odd == 0, core == 1)

    pl.semaphore_wait(barrier, 4 + groups - 1)
    for j in range(CHUNKS):
        far(j).start()

        @pl.when(odd == 0)
        def _():
            near(j).start()

        @pl.when(core == 0)
        def _():
            twin_own(j).start()

    acc[...] = jnp.zeros_like(acc)

    def span(slot, j, start, width):
        f = bufs[slot, j, probes:, :]
        p = bufs[slot, j, :probes, :]
        for t in range(width // TILE):
            cols = pl.ds(start + t * TILE, TILE)
            dist = lax.dot_general(f, feat[:, cols], (((0,), (0,)), ((), ())),
                                   preferred_element_type=jnp.float32)
            ker = lax.rsqrt(dist.astype(jnp.bfloat16))
            acc[:, cols] += jnp.dot(p, ker, preferred_element_type=jnp.float32)

    def unit(slot, j):
        span(slot, j, 0, sensors)

    def own(j, _):
        unit(0, j)
        return 0

    lax.fori_loop(0, CHUNKS, own, 0)

    def middle(j, _):
        @pl.when(j < CHUNKS)
        def _():
            arrived(4, j)
            twin_four(j).start()

            @pl.when(odd == 1)
            def _():
                near(j).start()

            @pl.when(relays)
            def _():
                relay_near(j).start()

        @pl.when(j >= 1)
        def _():
            arrived(2, j - 1)
            twin_two(j - 1).start()

            @pl.when(relays)
            def _():
                relay_far(j - 1).start()

            unit(2, j - 1)
            arrived(1 + 2 * core, j - 1)
            unit(1 + 2 * core, j - 1)

        @pl.when(j < CHUNKS)
        def _():
            unit(4, j)
            arrived(3 + 2 * core, j)
            unit(3 + 2 * core, j)
        return 0

    lax.fori_loop(0, CHUNKS + 1, middle, 0)

    last = 5 - 4 * core

    def fetch(j):
        @pl.when(core == 1)
        def _():
            arrived(6, j)
            twin_six(j).start()
        arrived(last, j)

    def final(j, _):
        fetch(j)
        unit(last, j)
        return 0

    lax.fori_loop(0, CHUNKS - 1, final, 0)
    fetch(CHUNKS - 1)

    def swap(q, k):
        return pltpu.make_async_remote_copy(
            src_ref=part.at[q, k - 1],
            dst_ref=got.at[q, k - 1],
            send_sem=psend_sem.at[q, k - 1],
            recv_sem=precv_sem.at[q, k - 1],
            device_id=((grp + k) % groups, me),
            device_id_type=MESH,
        )

    for q in range(QUARTERS):
        cols = pl.ds(q * quarter, quarter)
        span(last, CHUNKS - 1, q * quarter, quarter)
        for k in range(1, groups):
            take = pl.ds(pl.multiple_of(((grp + k) % groups) * rows, 8), rows)
            part[q, k - 1] = (acc[take, cols] * scale).astype(jnp.bfloat16)
            swap(q, k).start()
    for q in range(QUARTERS):
        cols = pl.ds(q * quarter, quarter)
        total = acc[pl.ds(pl.multiple_of(grp * rows, 8), rows), cols] * scale
        for k in range(1, groups):
            swap(q, k).wait_recv()
            total = total + got[q, k - 1].astype(jnp.float32)
        out_ref[:, cols] = total
        for k in range(1, groups):
            swap(q, k).wait_send()

    for j in range(CHUNKS):
        far(j).wait_send()
        near(j).wait_send()
        twin_four(j).wait_send()
        twin_two(j).wait_send()

        @pl.when(relays)
        def _():
            relay_far(j).wait_send()
            relay_near(j).wait_send()

        @pl.when(core == 0)
        def _():
            twin_own(j).wait_send()

        @pl.when(core == 1)
        def _():
            twin_six(j).wait_send()


def shards(sensors, sources, weights, probes):
    groups = lax.axis_size("grp")
    n_blk = lax.axis_size("blk")
    n_src, n_probe = probes.shape
    n_sens = sensors.shape[1]
    chunk = n_src // CHUNKS
    rows = n_probe // groups
    quarter = n_sens // QUARTERS
    scale = 1.0 / math.sqrt(STEPS * n_src * groups)
    vmem = pl.BlockSpec(memory_space=pltpu.VMEM)
    return pl.pallas_call(
        functools.partial(body, groups, n_blk, scale),
        out_shape=jax.ShapeDtypeStruct((rows, n_sens), jnp.float32),
        in_specs=[vmem] * 4,
        out_specs=vmem,
        scratch_shapes=[
            pltpu.VMEM((SLOTS, CHUNKS, n_probe + FEAT, chunk), jnp.bfloat16),
            pltpu.VMEM((FEAT, n_sens), jnp.bfloat16),
            pltpu.VMEM((n_probe, n_sens), jnp.float32),
            pltpu.VMEM((QUARTERS, groups - 1, rows, quarter), jnp.bfloat16),
            pltpu.VMEM((QUARTERS, groups - 1, rows, quarter), jnp.bfloat16),
            pltpu.SemaphoreType.DMA((8, CHUNKS)),
            pltpu.SemaphoreType.DMA((SLOTS, CHUNKS)),
            pltpu.SemaphoreType.DMA((QUARTERS, groups - 1)),
            pltpu.SemaphoreType.DMA((QUARTERS, groups - 1)),
        ],
        compiler_params=pltpu.CompilerParams(collective_id=0, has_side_effects=True),
    )(sensors, sources, weights.reshape(1, n_src), probes)


def solution(mesh):
    in_specs = (P(None, "blk"), P(None, ("grp", "blk")), P(("grp", "blk")), P(("grp", "blk"), None))
    out_specs = P("grp", "blk")
    return jax.shard_map(shards, mesh=mesh, in_specs=in_specs, out_specs=out_specs, check_vma=False)
```

```python
import functools
import math

import jax
import jax.numpy as jnp
from jax import lax
from jax.experimental import pallas as pl
from jax.experimental.pallas import tpu as pltpu
from jax.sharding import PartitionSpec as P

STEPS = 6
SLOTS = STEPS + 1
EPS = 0.0025
FEAT = 16
CHUNKS = 4
QUARTERS = 4
TILE = 1024
MESH = pl.DeviceIdType.MESH


def pieces(x):
    hi = x.astype(jnp.bfloat16)
    rest = x - hi.astype(jnp.float32)
    mid = rest.astype(jnp.bfloat16)
    lo = (rest - mid.astype(jnp.float32)).astype(jnp.bfloat16)
    return [hi.astype(jnp.float32), mid.astype(jnp.float32), lo.astype(jnp.float32)]


def body(groups, n_blk, scale, sens_ref, src_ref, wgt_ref, prb_ref, out_ref,
         bufs, feat, acc, part, got, send_sem, recv_sem, psend_sem, precv_sem):
    chunk = bufs.shape[3]
    probes = prb_ref.shape[1]
    sensors = sens_ref.shape[1]
    rows = probes // groups
    quarter = sensors // QUARTERS
    chips = n_blk // 2

    grp = lax.axis_index("grp")
    me = lax.axis_index("blk")
    chip = me // 2
    core = me % 2
    odd = chip % 2
    ahead = 2 * ((chip + 2) % chips) + core
    behind = 2 * ((chip + chips - 2) % chips) + core
    peer = 2 * (chip + 1 - 2 * odd) + core
    twin = 2 * chip + 1 - core

    barrier = pltpu.get_barrier_semaphore()
    for other in (ahead, behind, peer, twin):
        pl.semaphore_signal(barrier, inc=1, device_id=(grp, other), device_id_type=MESH)
    for k in range(1, groups):
        pl.semaphore_signal(barrier, inc=1, device_id=((grp + k) % groups, me), device_id_type=MESH)

    for j in range(CHUNKS):
        cols = pl.ds(j * chunk, chunk)
        turned = jnp.transpose(prb_ref[cols, :].astype(jnp.float32))
        bufs[0, j, :probes, :] = (turned * wgt_ref[cols].astype(jnp.float32)[None, :]).astype(jnp.bfloat16)
        s = src_ref[:, cols].astype(jnp.float32)
        square = jnp.sum(s * s, axis=0, keepdims=True)
        one = jnp.ones((1, chunk), jnp.float32)
        bufs[0, j, probes:, :] = jnp.concatenate(
            [s, s, s] + pieces(square) + [one, one, one, 0.0 * one], axis=0
        ).astype(jnp.bfloat16)
    x = sens_ref[...]
    square = jnp.sum(x * x, axis=0, keepdims=True) + EPS
    one = jnp.ones((1, sensors), jnp.float32)
    feat[...] = jnp.concatenate(
        [-2.0 * p for p in pieces(x)] + [one, one, one] + pieces(square) + [0.0 * one], axis=0
    ).astype(jnp.bfloat16)

    def copy(kind, src_slot, dst_slot, j, other):
        return pltpu.make_async_remote_copy(
            src_ref=bufs.at[src_slot, j],
            dst_ref=bufs.at[dst_slot, j],
            send_sem=send_sem.at[kind, j],
            recv_sem=recv_sem.at[dst_slot, j],
            device_id=(grp, other),
            device_id_type=MESH,
        )

    def arrived(slot, j):
        copy(0, slot, slot, j, ahead).wait_recv()

    def far(j): return copy(0, 0, 4, j, ahead)
    def near(j): return copy(1, 4 * odd, 2, j, peer)
    def relay_far(j): return copy(2, 2, 6, j, ahead)
    def relay_near(j): return copy(3, 4, 6, j, peer)
    def twin_own(j): return copy(4, 0, 1, j, twin)
    def twin_four(j): return copy(5, 4, 5 - 2 * core, j, twin)
    def twin_two(j): return copy(6, 2, 3 - 2 * core, j, twin)
    def twin_six(j): return copy(7, 6, 5, j, twin)

    relays = jnp.logical_and(odd == 0, core == 1)

    pl.semaphore_wait(barrier, 4 + groups - 1)
    for j in range(CHUNKS):
        far(j).start()

        @pl.when(odd == 0)
        def _():
            near(j).start()

        @pl.when(core == 0)
        def _():
            twin_own(j).start()

    acc[...] = jnp.zeros_like(acc)

    def span(slot, j, start, width):
        f = bufs[slot, j, probes:, :]
        p = bufs[slot, j, :probes, :]
        tile = min(TILE, width)
        for t in range(width // tile):
            cols = pl.ds(start + t * tile, tile)
            dist = lax.dot_general(f, feat[:, cols], (((0,), (0,)), ((), ())),
                                   preferred_element_type=jnp.float32)
            ker = lax.rsqrt(dist.astype(jnp.bfloat16))
            acc[:, cols] += jnp.dot(p, ker, preferred_element_type=jnp.float32)

    def unit(slot, j):
        span(slot, j, 0, sensors)

    def own(j, _):
        unit(0, j)
        return 0

    lax.fori_loop(0, CHUNKS, own, 0)

    def got_four(j):
        arrived(4, j)
        twin_four(j).start()

        @pl.when(odd == 1)
        def _():
            near(j).start()

        @pl.when(relays)
        def _():
            relay_near(j).start()

    def got_two(j):
        arrived(2, j)
        twin_two(j).start()

        @pl.when(relays)
        def _():
            relay_far(j).start()

    def middle(j, _):
        @pl.when(j <= 1)
        def _():
            got_four(j)

        @pl.when(jnp.logical_and(j >= 1, j <= 2))
        def _():
            got_two(j - 1)

        @pl.when(j >= 1)
        def _():
            unit(2, j - 1)
            arrived(1 + 2 * core, j - 1)
            unit(1 + 2 * core, j - 1)

        @pl.when(jnp.logical_and(j >= 1, j + 1 < CHUNKS))
        def _():
            got_four(j + 1)

        @pl.when(jnp.logical_and(j >= 2, j < CHUNKS))
        def _():
            got_two(j)

        @pl.when(j < CHUNKS)
        def _():
            unit(4, j)
            arrived(3 + 2 * core, j)
            unit(3 + 2 * core, j)
        return 0

    lax.fori_loop(0, CHUNKS + 1, middle, 0)

    last = 5 - 4 * core

    @pl.when(core == 1)
    def _():
        for j in range(CHUNKS):
            arrived(6, j)
            twin_six(j).start()
    for j in range(CHUNKS):
        arrived(last, j)

    def swap(q, k):
        return pltpu.make_async_remote_copy(
            src_ref=part.at[q, k - 1],
            dst_ref=got.at[q, k - 1],
            send_sem=psend_sem.at[q, k - 1],
            recv_sem=precv_sem.at[q, k - 1],
            device_id=((grp + k) % groups, me),
            device_id_type=MESH,
        )

    for q in range(QUARTERS):
        cols = pl.ds(q * quarter, quarter)
        for j in range(CHUNKS):
            span(last, j, q * quarter, quarter)
        for k in range(1, groups):
            take = pl.ds(pl.multiple_of(((grp + k) % groups) * rows, 8), rows)
            part[q, k - 1] = (acc[take, cols] * scale).astype(jnp.bfloat16)
            swap(q, k).start()
    for q in range(QUARTERS):
        cols = pl.ds(q * quarter, quarter)
        total = acc[pl.ds(pl.multiple_of(grp * rows, 8), rows), cols] * scale
        for k in range(1, groups):
            swap(q, k).wait_recv()
            total = total + got[q, k - 1].astype(jnp.float32)
        out_ref[:, cols] = total
        for k in range(1, groups):
            swap(q, k).wait_send()

    for j in range(CHUNKS):
        far(j).wait_send()
        near(j).wait_send()
        twin_four(j).wait_send()
        twin_two(j).wait_send()

        @pl.when(relays)
        def _():
            relay_far(j).wait_send()
            relay_near(j).wait_send()

        @pl.when(core == 0)
        def _():
            twin_own(j).wait_send()

        @pl.when(core == 1)
        def _():
            twin_six(j).wait_send()


def shards(sensors, sources, weights, probes):
    groups = lax.axis_size("grp")
    n_blk = lax.axis_size("blk")
    n_src, n_probe = probes.shape
    n_sens = sensors.shape[1]
    chunk = n_src // CHUNKS
    rows = n_probe // groups
    quarter = n_sens // QUARTERS
    scale = 1.0 / math.sqrt(STEPS * n_src * groups)
    vmem = pl.BlockSpec(memory_space=pltpu.VMEM)
    return pl.pallas_call(
        functools.partial(body, groups, n_blk, scale),
        out_shape=jax.ShapeDtypeStruct((rows, n_sens), jnp.float32),
        in_specs=[vmem] * 4,
        out_specs=vmem,
        scratch_shapes=[
            pltpu.VMEM((SLOTS, CHUNKS, n_probe + FEAT, chunk), jnp.bfloat16),
            pltpu.VMEM((FEAT, n_sens), jnp.bfloat16),
            pltpu.VMEM((n_probe, n_sens), jnp.float32),
            pltpu.VMEM((QUARTERS, groups - 1, rows, quarter), jnp.bfloat16),
            pltpu.VMEM((QUARTERS, groups - 1, rows, quarter), jnp.bfloat16),
            pltpu.SemaphoreType.DMA((8, CHUNKS)),
            pltpu.SemaphoreType.DMA((SLOTS, CHUNKS)),
            pltpu.SemaphoreType.DMA((QUARTERS, groups - 1)),
            pltpu.SemaphoreType.DMA((QUARTERS, groups - 1)),
        ],
        compiler_params=pltpu.CompilerParams(collective_id=0, has_side_effects=True),
    )(sensors, sources, weights, probes)


def solution(mesh):
    in_specs = (P(None, "blk"), P(None, ("grp", "blk")), P(("grp", "blk")), P(("grp", "blk"), None))
    out_specs = P("grp", "blk")
    return jax.shard_map(shards, mesh=mesh, in_specs=in_specs, out_specs=out_specs, check_vma=False)
```
